256 devices in a mesh: pp: 4 (over x_hi, core), tp: 16 (over z, x_lo), dp: 4 (over y).
Axes of the slice: x: 4 (x_hi: 2, x_lo: 2; x = x_hi * 2 + x_lo), y: 4, z: 8, core: 2. Of those that a mesh axis runs over, the one named last changes fastest.
Arguments:
- layer_input: bfloat16 [4, 4, 128, 4096], P('pp', 'dp', 'tp'), may hold values from -4 to 4
- gate_pre: bfloat16 [4, 4, 128, 14784], P('pp', 'dp', None, 'tp'), may hold values from -8 to 8
- up_pre: bfloat16 [4, 4, 128, 14784], P('pp', 'dp', None, 'tp'), may hold values from -6 to 6
- hidden_grad: bfloat16 [4, 4, 128, 14784], P('pp', 'dp', None, 'tp'), may hold values from -0.59765625 to 0.59765625
- gate_weight: bfloat16 [4, 4096, 14784], P('pp', 'dp', 'tp'), may hold values from -0.09375 to 0.09375
Outputs:
- passed_grad: bfloat16 [4, 4, 128, 4096], P('pp', 'dp', 'tp')
- gate_weight_grad: bfloat16 [4, 4096, 14784], P('pp', 'dp', 'tp')
The draws below stay inside these ranges and needn't reach their ends.
All inputs are finite; a program needn't handle non-finite values.
Results may differ from the reference program's by a relative error of at most 0.018.
Values may be sent and summed in bfloat16 or wider, within the bound.
A program may use at most 64 MiB of HBM per device.

```python
import jax
import jax.numpy as jnp
from jax import lax

D = 4096
FF = 14784
GROUP_TOKENS = 128
SECTIONS = 4
REPLICAS = 4
N_PP = 4
N_DP = 4


def spiked(drawn, stream_key, source, target, parts, factor):
    def block_of(dim):
        return (jnp.arange(drawn.shape[dim]) // (drawn.shape[dim] // parts)).reshape((-1,) + (1,) * (drawn.ndim - 1 - dim))

    first = jax.random.permutation(stream_key, parts)[block_of(target)]
    second = (block_of(target) + parts // 2) % parts
    return jnp.where((block_of(source) == first) | (block_of(source) == second), factor * drawn, drawn)


def levels(own_key, extent, pieces, smallest, high):
    loudness = 1.0
    for dim, parts in pieces:
        draws = jax.random.uniform(jax.random.fold_in(jax.random.fold_in(own_key, 6), dim), (parts,), jnp.float32, smallest / len(pieces), high / len(pieces))
        loudness = loudness * jnp.repeat(jnp.exp(draws), extent[dim] // parts).reshape((-1,) + (1,) * (len(extent) - 1 - dim))
    return loudness


def centred(stream_key, extent, width, bound, pieces=(), kind=jnp.bfloat16):
    values = jax.random.normal(stream_key, extent, jnp.float32) * width
    if len(pieces) > 0:
        values = levels(stream_key, extent, pieces, -0.22, 0.18) * values
    return jnp.clip(values, min=-bound, max=bound).astype(kind)


def heavy_noise(rng, shape, scale, limit, cuts, heavy, held_as=jnp.bfloat16):
    result = scale * jax.random.normal(rng, shape, jnp.float32)
    if cuts:
        result = result * levels(rng, shape, cuts, -0.22, 0.18)
    return jnp.clip(spiked(result, jax.random.fold_in(rng, 3), *heavy), -limit, limit).astype(held_as)


def setup_inputs(seed: int = 0) -> dict:
    keys = jax.random.split(jax.random.key(seed), 6)
    layer_input = heavy_noise(keys[0], (SECTIONS, REPLICAS, GROUP_TOKENS, D), 0.5, 4.0, ((0, 4), (1, 4), (2, 16)), (1, 3, 4, 2.0))
    gate_pre = centred(keys[1], (SECTIONS, REPLICAS, GROUP_TOKENS, FF), 1.5, 8.0, ((0, 4), (1, 4), (3, 16)))
    up_pre = centred(keys[2], (SECTIONS, REPLICAS, GROUP_TOKENS, FF), 1.0, 6.0, ((0, 4), (1, 4), (3, 16)))
    hidden_grad = centred(keys[3], (SECTIONS, REPLICAS, GROUP_TOKENS, FF), 0.1, 0.59765625, ((0, 4), (1, 4), (3, 16)))
    gate_weight = centred(keys[4], (SECTIONS, D, FF), D ** -0.5, 0.09375, ((0, 4), (1, 4), (2, 16)))
    return {"layer_input": layer_input, "gate_pre": gate_pre, "up_pre": up_pre, "hidden_grad": hidden_grad, "gate_weight": gate_weight}


def local_grad(gate_act, up_act, hidden):
    gate_val = gate_act.astype(jnp.float32)
    up_val = up_act.astype(jnp.float32)
    hidden_val = hidden.astype(jnp.float32)
    logistic = jax.nn.sigmoid(gate_val)
    return (hidden_val * up_val * logistic * (1.0 + gate_val * (1.0 - logistic))).astype(jnp.bfloat16)

def reference(layer_input, gate_pre, up_pre, hidden_grad, gate_weight):
    input_list = []
    gate_list = []
    for which_section in range(N_PP):
        gate_total = jnp.zeros((D, FF), jnp.float32)
        replica_grads = []
        for replica in range(N_DP):
            gate_grad = local_grad(gate_pre[which_section, replica], up_pre[which_section, replica], hidden_grad[which_section, replica])
            summed = jnp.dot(gate_grad, gate_weight[which_section].T, preferred_element_type=jnp.float32)
            replica_grads.append(summed.astype(jnp.bfloat16))
            tokens_in = layer_input[which_section, replica]
            gate_term = lax.optimization_barrier(jnp.dot(tokens_in.T, gate_grad, preferred_element_type=jnp.float32).astype(jnp.bfloat16))
            gate_total = gate_total + gate_term.astype(jnp.float32)
        input_list.append(jnp.stack(replica_grads))
        gate_list.append(gate_total.astype(jnp.bfloat16))
    zeros_last = jnp.zeros_like(input_list[0])
    passed_grad = jnp.stack(input_list[1:] + [zeros_last])
    return (passed_grad, jnp.stack(gate_list))
```

```python
import jax
import jax.numpy as jnp
from jax import lax
from jax.experimental import pallas as pl
from jax.experimental.pallas import tpu as pltpu
from jax.sharding import PartitionSpec as P

MESH = pl.DeviceIdType.MESH
F32 = jnp.float32
BF16 = jnp.bfloat16


def kernel(
    x_hbm, gate_hbm, up_hbm, hid_hbm, w_hbm,
    dx_ref, dw_ref,
    gate_v, up_v, hid_v, w_v, g_all, x_all, x_mat, part, ring, fin, landed,
    load_sem, xs, xr, ps, pr, gs, gr, ags, agr, rss, rsr, fs, fr,
):
    p, t, y = lax.axis_index("pp"), lax.axis_index("tp"), lax.axis_index("dp")
    n_pp, n_dp = lax.axis_size("pp"), lax.axis_size("dp")
    z, xl = t // 2, lax.rem(t, 2)
    nz = 8
    hidden = gate_hbm.shape[0]
    half = g_all.shape[2]
    rest = hidden - half
    cols = w_hbm.shape[1]
    hc = cols // 2

    def zmod(v):
        return lax.rem(v + 2 * nz, nz)

    def ymod(v):
        return lax.rem(v + 2 * n_dp, n_dp)

    def at_z(d):
        return (p, zmod(z + d) * 2 + xl, y)

    def at_y(d):
        return (p, t, ymod(y + d))

    partner = (p, t + 1 - 2 * xl, y)

    def remote(src, dst, ssem, rsem, dev):
        return pltpu.make_async_remote_copy(
            src_ref=src, dst_ref=dst, send_sem=ssem, recv_sem=rsem,
            device_id=dev, device_id_type=MESH,
        )

    loads = [
        pltpu.make_async_copy(gate_hbm, gate_v, load_sem.at[0]),
        pltpu.make_async_copy(up_hbm, up_v, load_sem.at[1]),
        pltpu.make_async_copy(hid_hbm, hid_v, load_sem.at[2]),
        pltpu.make_async_copy(w_hbm, w_v, load_sem.at[3]),
        pltpu.make_async_copy(
            x_hbm.at[:, pl.ds(pl.multiple_of(y * cols, 128), cols)],
            x_all.at[z, xl, y], load_sem.at[4]),
    ]
    for c in loads:
        c.start()

    barrier = pltpu.get_barrier_semaphore()
    peers = [at_y(1), at_y(2), at_y(3), at_z(1), at_z(-1), partner]
    for d in peers:
        pl.semaphore_signal(barrier, inc=1, device_id=d, device_id_type=MESH)

    @pl.when(p < n_pp - 1)
    def _():
        for j in range(4):
            for xq in range(2):
                pl.semaphore_signal(
                    barrier, inc=1, device_id=(p + 1, z * 2 + xq, j), device_id_type=MESH)

    pl.semaphore_wait(barrier, jnp.where(p > 0, len(peers) + 8, len(peers)))

    sends = []

    def go(c):
        c.start()
        sends.append(c)

    def x_copy(k):
        j = ymod(y + k)
        return remote(
            x_hbm.at[:, pl.ds(pl.multiple_of(j * cols, 128), cols)],
            x_all.at[z, xl, y], xs.at[k - 1], xr.at[k - 1], at_y(k))

    for k in (1, 3, 2):
        go(x_copy(k))

    for c in loads[:3]:
        c.wait()
    for h, (lo, n) in enumerate(((0, half), (half, rest))):
        rows = pl.ds(lo, n)
        g = gate_v[rows, :].astype(F32)
        u = up_v[rows, :].astype(F32)
        d = hid_v[rows, :].astype(F32)
        s = jax.nn.sigmoid(g)
        v = d * u * s * (1.0 + g * (1.0 - s))
        if n < half:
            v = jnp.concatenate([v, jnp.zeros((half - n, v.shape[1]), F32)], axis=0)
        g_all[y, h] = v.astype(BF16)

    def g_copy(plus, k):
        if plus:
            owner, h, dev = ((y, 0), (y, 1), (ymod(y - 1), 0))[k] + (at_y(1),)
        else:
            owner, h, dev = ((y, 1), (y, 0), (ymod(y + 1), 1))[k] + (at_y(-1),)
        i = 0 if plus else 1
        ref = g_all.at[owner, h]
        return remote(ref, ref, gs.at[i, k], gr.at[i, k], dev)

    for k in (0, 1):
        go(g_copy(True, k))
        go(g_copy(False, k))

    def rep(ri):
        return ymod(y + (0, 1, 3, 2)[ri])

    def product(ri):
        r = rep(ri)
        g = jnp.concatenate([g_all[r, 0], g_all[r, 1]], axis=0)[:hidden]
        for q in range(2):
            c = pl.ds(q * hc, hc)
            acc = lax.dot_general(
                g, w_v[:, c], (((0,), (0,)), ((), ())), preferred_element_type=F32)
            part[ri, :, :, c] = acc.astype(BF16).reshape(nz, 16, hc)

    def lanes(plus):
        return pl.ds(0, hc) if plus else pl.ds(hc, hc)

    def rs_copy(plus, ri, s):
        i, sign = (0, 1) if plus else (1, -1)
        src = part.at[ri, zmod(z + sign * (5 - s))]
        dst = ring.at[i, ri, s - 1]
        if s == 1:
            src, dst = src.at[:, lanes(plus)], dst.at[:, lanes(plus)]
        return remote(src, dst, rss.at[i, ri, s - 1], rsr.at[i, ri, s - 1], at_z(sign))

    def rs_start(ri):
        for plus in (True, False):
            go(rs_copy(plus, ri, 1))

    def rs_next(ri, s):
        for plus in (True, False):
            i, sign = (0, 1) if plus else (1, -1)
            rs_copy(plus, ri, s - 1).wait_recv()
            d = zmod(z + sign * (5 - s))
            c = lanes(plus) if s == 2 else pl.ds(0, cols)
            part[ri, d, :, c] = (
                part[ri, d, :, c].astype(F32) + ring[i, ri, s - 2, :, c].astype(F32)
            ).astype(BF16)
            go(rs_copy(plus, ri, s))

    def fin_copy(ri, xq):
        return remote(
            fin.at[ri, xq], landed.at[y, xl], fs.at[ri, xq], fr.at[y, xl],
            (jnp.maximum(p - 1, 0), z * 2 + xq, rep(ri)))

    def rs_end(ri):
        for plus in (True, False):
            rs_copy(plus, ri, 4).wait_recv()
        v = (
            part[ri, z].astype(F32) + ring[0, ri, 3].astype(F32) + ring[1, ri, 3].astype(F32)
        )
        v = v.reshape(2, 8, cols).astype(BF16)
        for xq in range(2):
            fin[ri, xq] = v[xq]

        @pl.when(p > 0)
        def _():
            for xq in range(2):
                fin_copy(ri, xq).start()

    def pair_copy():
        ref = x_all.at[z, xl]
        return remote(ref, ref, ps.at[0], pr.at[0], partner)

    def ag_copy(plus, slot, s):
        i, sign = (0, 1) if plus else (1, -1)
        col = xl if slot == 0 else 1 - xl
        ref = x_all.at[zmod(z - sign * (s - 1)), col]
        if s == 4:
            ref = ref.at[pl.ds(0, 2)] if plus else ref.at[pl.ds(2, 2)]
        return remote(
            ref, ref, ags.at[i, slot, s - 1], agr.at[i, slot, s - 1], at_z(sign))

    def ag_start(slot):
        for plus in (True, False):
            go(ag_copy(plus, slot, 1))

    def ag_next(slot, s):
        for plus in (True, False):
            ag_copy(plus, slot, s - 1).wait_recv()
            go(ag_copy(plus, slot, s))

    def ag_end(slot):
        for plus in (True, False):
            ag_copy(plus, slot, 4).wait_recv()

    loads[3].wait()
    product(0)
    rs_start(0)

    loads[4].wait()
    for k in (1, 3, 2):
        x_copy(k).wait_recv()
    go(pair_copy())
    ag_start(0)

    g_copy(True, 0).wait_recv()
    go(g_copy(True, 2))
    g_copy(False, 0).wait_recv()
    go(g_copy(False, 2))

    rs_next(0, 2)
    pair_copy().wait_recv()
    ag_start(1)
    ag_next(0, 2)

    g_copy(True, 1).wait_recv()
    g_copy(False, 1).wait_recv()
    product(1)
    rs_start(1)
    product(2)
    rs_start(2)
    rs_next(0, 3)
    ag_next(1, 2)

    g_copy(True, 2).wait_recv()
    g_copy(False, 2).wait_recv()
    product(3)
    rs_start(3)
    rs_next(1, 2)
    rs_next(2, 2)
    rs_next(0, 4)
    ag_next(0, 3)
    rs_next(3, 2)
    rs_next(1, 3)
    rs_next(2, 3)
    rs_end(0)
    ag_next(1, 3)
    rs_next(3, 3)
    rs_next(1, 4)
    rs_next(2, 4)
    ag_next(0, 4)
    rs_next(3, 4)
    ag_next(1, 4)
    rs_end(1)
    rs_end(2)
    rs_end(3)

    ag_end(0)
    ag_end(1)
    for r in range(4):
        x_mat[pl.ds(r * 128, 128), :] = (
            x_all[:, :, r].astype(F32).reshape(128, cols).astype(BF16))
    for lo in range(0, hidden, 128):
        n = min(128, hidden - lo)
        pieces = []
        for r in range(4):
            if lo + n <= half:
                pieces.append(g_all[r, 0, pl.ds(lo, n), :])
            elif lo >= half:
                pieces.append(g_all[r, 1, pl.ds(lo - half, n), :])
            else:
                pieces.append(jnp.concatenate(
                    [g_all[r, 0, pl.ds(lo, half - lo), :],
                     g_all[r, 1, pl.ds(0, lo + n - half), :]], axis=0))
        g = jnp.concatenate(pieces, axis=1)
        dw_ref[pl.ds(lo, n), :] = jnp.dot(
            g, x_mat[...], preferred_element_type=F32).astype(BF16)

    @pl.when(p < n_pp - 1)
    def _():
        for j in range(4):
            for xq in range(2):
                remote(
                    landed.at[j, xq], landed.at[j, xq], fs.at[0, 0], fr.at[j, xq],
                    partner).wait_recv()
            dx_ref[:, pl.ds(j * cols, cols)] = (
                landed[j, 0].astype(F32) + landed[j, 1].astype(F32)).astype(BF16)

    @pl.when(p == n_pp - 1)
    def _():
        dx_ref[...] = jnp.zeros_like(dx_ref)

    for c in sends:
        c.wait_send()

    @pl.when(p > 0)
    def _():
        for ri in range(4):
            for xq in range(2):
                fin_copy(ri, xq).wait_send()


def on_device(layer_input, gate_pre, up_pre, hidden_grad, gate_weight):
    x = layer_input[0, 0]
    gate, up, hid = (jnp.swapaxes(v[0, 0], 0, 1) for v in (gate_pre, up_pre, hidden_grad))
    w = jnp.swapaxes(gate_weight[0], 0, 1)
    hidden, toks = gate.shape
    cols = w.shape[1]
    half = (hidden // 2 + 15) // 16 * 16
    vm = pltpu.VMEM
    dma = pltpu.SemaphoreType.DMA
    dx, dw = pl.pallas_call(
        kernel,
        name="section",
        out_shape=(
            jax.ShapeDtypeStruct(x.shape, BF16),
            jax.ShapeDtypeStruct((hidden, cols), BF16),
        ),
        in_specs=[pl.BlockSpec(memory_space=pl.ANY)] * 5,
        out_specs=[pl.BlockSpec(memory_space=pltpu.VMEM)] * 2,
        scratch_shapes=[
            vm((hidden, toks), BF16), vm((hidden, toks), BF16), vm((hidden, toks), BF16),
            vm((hidden, cols), BF16),
            vm((4, 2, half, toks), BF16),
            vm((8, 2, 4, 8, cols), BF16),
            vm((512, cols), BF16),
            vm((4, 8, 16, cols), BF16),
            vm((2, 4, 4, 16, cols), BF16),
            vm((4, 2, 8, cols), BF16),
            vm((4, 2, 8, cols), BF16),
            dma((5,)), dma((3,)), dma((3,)), dma((1,)), dma((1,)),
            dma((2, 3)), dma((2, 3)),
            dma((2, 2, 4)), dma((2, 2, 4)),
            dma((2, 4, 4)), dma((2, 4, 4)),
            dma((4, 2)), dma((4, 2)),
        ],
        compiler_params=pltpu.CompilerParams(
            collective_id=0, has_side_effects=True, vmem_limit_bytes=40 << 20),
    )(x, gate, up, hid, w)
    return dx[None, None], jnp.swapaxes(dw, 0, 1)[None]


def solution(mesh):
    return jax.shard_map(
        on_device,
        mesh=mesh,
        in_specs=(
            P("pp", "dp", "tp", None),
            P("pp", "dp", None, "tp"),
            P("pp", "dp", None, "tp"),
            P("pp", "dp", None, "tp"),
            P("pp", "dp", "tp"),
        ),
        out_specs=(P("pp", "dp", "tp", None), P("pp", "dp", "tp")),
        check_vma=False,
    )
```

```python
import jax
import jax.numpy as jnp
from jax import lax
from jax.experimental import pallas as pl
from jax.experimental.pallas import tpu as pltpu
from jax.sharding import PartitionSpec as P

MESH = pl.DeviceIdType.MESH
F32 = jnp.float32
BF16 = jnp.bfloat16


def kernel(
    x_hbm, gate_hbm, up_hbm, hid_hbm, w_hbm,
    dx_ref, dw_ref,
    gate_v, up_v, hid_v, w_v, x_v, g_all, x_all, x_mat, part, ring, fin, landed,
    load_sem, xs, xr, ps, pr, gs, gr, ags, agr, rss, rsr, fs, fr,
):
    p, t, y = lax.axis_index("pp"), lax.axis_index("tp"), lax.axis_index("dp")
    n_pp, n_dp = lax.axis_size("pp"), lax.axis_size("dp")
    z, xl = t // 2, lax.rem(t, 2)
    nz = 8
    hidden = gate_hbm.shape[0]
    half = g_all.shape[2]
    rest = hidden - half
    cols = w_hbm.shape[1]
    hc = cols // 2

    def zmod(v):
        return lax.rem(v + 2 * nz, nz)

    def ymod(v):
        return lax.rem(v + 2 * n_dp, n_dp)

    def at_z(d):
        return (p, zmod(z + d) * 2 + xl, y)

    def at_y(d):
        return (p, t, ymod(y + d))

    partner = (p, t + 1 - 2 * xl, y)

    def remote(src, dst, ssem, rsem, dev):
        return pltpu.make_async_remote_copy(
            src_ref=src, dst_ref=dst, send_sem=ssem, recv_sem=rsem,
            device_id=dev, device_id_type=MESH,
        )

    loads = [
        pltpu.make_async_copy(gate_hbm, gate_v, load_sem.at[0]),
        pltpu.make_async_copy(up_hbm, up_v, load_sem.at[1]),
        pltpu.make_async_copy(hid_hbm, hid_v, load_sem.at[2]),
        pltpu.make_async_copy(w_hbm, w_v, load_sem.at[3]),
        pltpu.make_async_copy(
            x_hbm.at[:, pl.ds(pl.multiple_of(y * cols, 128), cols)],
            x_all.at[z, xl, y], load_sem.at[4]),
        pltpu.make_async_copy(x_hbm, x_v, load_sem.at[5]),
    ]
    for i in (5, 0, 1, 2, 4, 3):
        loads[i].start()

    barrier = pltpu.get_barrier_semaphore()
    peers = [at_y(1), at_y(2), at_y(3), at_z(1), at_z(-1), at_z(2), at_z(-2), partner]
    for d in peers:
        pl.semaphore_signal(barrier, inc=1, device_id=d, device_id_type=MESH)

    @pl.when(p < n_pp - 1)
    def _():
        for j in range(4):
            for xq in range(2):
                pl.semaphore_signal(
                    barrier, inc=1, device_id=(p + 1, z * 2 + xq, j), device_id_type=MESH)

    pl.semaphore_wait(barrier, jnp.where(p > 0, len(peers) + 8, len(peers)))

    sends = []

    def go(c):
        c.start()
        sends.append(c)

    def x_copy(k):
        j = ymod(y + k)
        return remote(
            x_v.at[:, pl.ds(pl.multiple_of(j * cols, 128), cols)],
            x_all.at[z, xl, y], xs.at[k - 1], xr.at[k - 1], at_y(k))

    loads[5].wait()
    for k in (2, 1, 3):
        go(x_copy(k))

    for c in loads[:3]:
        c.wait()
    for h, (lo, n) in enumerate(((0, half), (half, rest))):
        rows = pl.ds(lo, n)
        g = gate_v[rows, :].astype(F32)
        u = up_v[rows, :].astype(F32)
        d = hid_v[rows, :].astype(F32)
        s = jax.nn.sigmoid(g)
        v = d * u * s * (1.0 + g * (1.0 - s))
        if n < half:
            v = jnp.concatenate([v, jnp.zeros((half - n, v.shape[1]), F32)], axis=0)
        g_all[y, h] = v.astype(BF16)

    def g_copy(plus, k):
        if plus:
            owner, h, dev = ((y, 0), (y, 1), (ymod(y - 1), 0))[k] + (at_y(1),)
        else:
            owner, h, dev = ((y, 1), (y, 0), (ymod(y + 1), 1))[k] + (at_y(-1),)
        i = 0 if plus else 1
        ref = g_all.at[owner, h]
        return remote(ref, ref, gs.at[i, k], gr.at[i, k], dev)

    for k in (0, 1):
        go(g_copy(True, k))
        go(g_copy(False, k))

    def rep(ri):
        return ymod(y + (0, 1, 3, 2)[ri])

    def product(ri):
        r = rep(ri)
        g = jnp.concatenate([g_all[r, 0], g_all[r, 1]], axis=0)[:hidden]
        for q in range(2):
            c = pl.ds(q * hc, hc)
            acc = lax.dot_general(
                g, w_v[:, c], (((0,), (0,)), ((), ())), preferred_element_type=F32)
            part[ri, :, :, c] = acc.astype(BF16).reshape(nz, 16, hc)

    def lanes(plus):
        return pl.ds(0, hc) if plus else pl.ds(hc, hc)

    def rs_copy(plus, ri, kind):
        i, sign = (0, 1) if plus else (1, -1)
        dest, hop = ((3, 1), (4, 2), (1, 1), (2, 2))[kind]
        src = part.at[ri, zmod(z + sign * dest)]
        dst = ring.at[i, ri, kind]
        if kind == 1:
            src, dst = src.at[:, lanes(plus)], dst.at[:, lanes(plus)]
        return remote(src, dst, rss.at[i, ri, kind], rsr.at[i, ri, kind], at_z(sign * hop))

    def rs_send(ri, *kinds):
        for kind in kinds:
            for plus in (True, False):
                go(rs_copy(plus, ri, kind))

    def rs_mid(ri):
        for plus in (True, False):
            i, sign = (0, 1) if plus else (1, -1)
            for kind in (0, 1):
                rs_copy(plus, ri, kind).wait_recv()
            d = zmod(z + sign * 2)
            for q in range(2):
                c = pl.ds(q * hc, hc)
                v = part[ri, d, :, c].astype(F32) + ring[i, ri, 0, :, c].astype(F32)
                if plus == (q == 0):
                    v = v + ring[i, ri, 1, :, c].astype(F32)
                part[ri, d, :, c] = v.astype(BF16)
            go(rs_copy(plus, ri, 3))

    def fin_copy(ri, xq):
        return remote(
            fin.at[ri, xq], landed.at[y, xl], fs.at[ri, xq], fr.at[y, xl],
            (jnp.maximum(p - 1, 0), z * 2 + xq, rep(ri)))

    def rs_end(ri):
        v = part[ri, z].astype(F32)
        for kind in (2, 3):
            for plus in (True, False):
                rs_copy(plus, ri, kind).wait_recv()
                v = v + ring[0 if plus else 1, ri, kind].astype(F32)
        v = v.reshape(2, 8, cols).astype(BF16)
        for xq in range(2):
            fin[ri, xq] = v[xq]

        @pl.when(p > 0)
        def _():
            for xq in range(2):
                fin_copy(ri, xq).start()

    def pair_copy(k):
        ref = x_all.at[zmod(z + k), xl]
        return remote(ref, ref, ps.at[k % nz], pr.at[k % nz], partner)

    def ag_copy(plus, kind):
        i, sign = (0, 1) if plus else (1, -1)
        origin, hop = ((0, 1), (0, 2), (-2, 1), (-2, 2))[kind]
        ref = x_all.at[zmod(z + sign * origin), xl]
        if kind == 3:
            ref = ref.at[pl.ds(0, 2)] if plus else ref.at[pl.ds(2, 2)]
        return remote(ref, ref, ags.at[i, kind], agr.at[i, kind], at_z(sign * hop))

    def ag_send(*kinds):
        for kind in kinds:
            for plus in (True, False):
                go(ag_copy(plus, kind))

    def ag_wait(kind):
        for plus in (True, False):
            ag_copy(plus, kind).wait_recv()

    loads[3].wait()
    product(0)
    rs_send(0, 1, 0)

    loads[4].wait()
    for k in (1, 3, 2):
        x_copy(k).wait_recv()
    ag_send(1, 0)
    go(pair_copy(0))
    rs_send(0, 2)

    rs_mid(0)
    g_copy(True, 0).wait_recv()
    go(g_copy(True, 2))
    g_copy(False, 0).wait_recv()
    go(g_copy(False, 2))

    ag_wait(1)
    ag_send(3, 2)
    go(pair_copy(2))
    go(pair_copy(-2))

    g_copy(True, 1).wait_recv()
    g_copy(False, 1).wait_recv()
    product(1)
    rs_send(1, 1, 0)
    product(2)
    rs_send(2, 1, 0)
    ag_wait(0)
    go(pair_copy(1))
    go(pair_copy(-1))
    rs_end(0)

    g_copy(True, 2).wait_recv()
    g_copy(False, 2).wait_recv()
    product(3)
    rs_send(3, 1, 0)
    rs_send(1, 2)
    rs_send(2, 2)
    rs_send(3, 2)
    rs_mid(1)
    rs_mid(2)
    ag_wait(2)
    go(pair_copy(3))
    go(pair_copy(-3))
    ag_wait(3)
    go(pair_copy(4))
    rs_mid(3)
    rs_end(1)
    rs_end(2)
    rs_end(3)

    for k in range(nz):
        pair_copy(k).wait_recv()
    for r in range(4):
        x_mat[pl.ds(r * 128, 128), :] = (
            x_all[:, :, r].astype(F32).reshape(128, cols).astype(BF16))
    for lo in range(0, hidden, 128):
        n = min(128, hidden - lo)
        pieces = []
        for r in range(4):
            if lo + n <= half:
                pieces.append(g_all[r, 0, pl.ds(lo, n), :])
            elif lo >= half:
                pieces.append(g_all[r, 1, pl.ds(lo - half, n), :])
            else:
                pieces.append(jnp.concatenate(
                    [g_all[r, 0, pl.ds(lo, half - lo), :],
                     g_all[r, 1, pl.ds(0, lo + n - half), :]], axis=0))
        g = jnp.concatenate(pieces, axis=1)
        dw_ref[pl.ds(lo, n), :] = jnp.dot(
            g, x_mat[...], preferred_element_type=F32).astype(BF16)

    @pl.when(p < n_pp - 1)
    def _():
        for j in range(4):
            for xq in range(2):
                remote(
                    landed.at[j, xq], landed.at[j, xq], fs.at[0, 0], fr.at[j, xq],
                    partner).wait_recv()
            dx_ref[:, pl.ds(j * cols, cols)] = (
                landed[j, 0].astype(F32) + landed[j, 1].astype(F32)).astype(BF16)

    @pl.when(p == n_pp - 1)
    def _():
        dx_ref[...] = jnp.zeros_like(dx_ref)

    for c in sends:
        c.wait_send()

    @pl.when(p > 0)
    def _():
        for ri in range(4):
            for xq in range(2):
                fin_copy(ri, xq).wait_send()


def on_device(layer_input, gate_pre, up_pre, hidden_grad, gate_weight):
    x = layer_input[0, 0]
    gate, up, hid = (jnp.swapaxes(v[0, 0], 0, 1) for v in (gate_pre, up_pre, hidden_grad))
    w = jnp.swapaxes(gate_weight[0], 0, 1)
    hidden, toks = gate.shape
    cols = w.shape[1]
    half = (hidden // 2 + 15) // 16 * 16
    vm = pltpu.VMEM
    dma = pltpu.SemaphoreType.DMA
    dx, dw = pl.pallas_call(
        kernel,
        name="section",
        out_shape=(
            jax.ShapeDtypeStruct(x.shape, BF16),
            jax.ShapeDtypeStruct((hidden, cols), BF16),
        ),
        in_specs=[pl.BlockSpec(memory_space=pltpu.HBM)] * 5,
        out_specs=[pl.BlockSpec(memory_space=pltpu.VMEM)] * 2,
        scratch_shapes=[
            vm((hidden, toks), BF16), vm((hidden, toks), BF16), vm((hidden, toks), BF16),
            vm((hidden, cols), BF16),
            vm(x.shape, BF16),
            vm((4, 2, half, toks), BF16),
            vm((8, 2, 4, 8, cols), BF16),
            vm((512, cols), BF16),
            vm((4, 8, 16, cols), BF16),
            vm((2, 4, 4, 16, cols), BF16),
            vm((4, 2, 8, cols), BF16),
            vm((4, 2, 8, cols), BF16),
            dma((6,)), dma((3,)), dma((3,)), dma((8,)), dma((8,)),
            dma((2, 3)), dma((2, 3)),
            dma((2, 4)), dma((2, 4)),
            dma((2, 4, 4)), dma((2, 4, 4)),
            dma((4, 2)), dma((4, 2)),
        ],
        compiler_params=pltpu.CompilerParams(
            collective_id=0, has_side_effects=True, vmem_limit_bytes=40 << 20),
    )(*(pltpu.with_memory_space_constraint(v, pltpu.HBM) for v in (x, gate, up, hid, w)))
    return dx[None, None], jnp.swapaxes(dw, 0, 1)[None]


def solution(mesh):
    return jax.shard_map(
        on_device,
        mesh=mesh,
        in_specs=(
            P("pp", "dp", "tp", None),
            P("pp", "dp", None, "tp"),
            P("pp", "dp", None, "tp"),
            P("pp", "dp", None, "tp"),
            P("pp", "dp", "tp"),
        ),
        out_specs=(P("pp", "dp", "tp", None), P("pp", "dp", "tp")),
        check_vma=False,
    )
```

```python
import jax
import jax.numpy as jnp
from jax import lax
from jax.experimental import pallas as pl
from jax.experimental.pallas import tpu as pltpu
from jax.sharding import PartitionSpec as P

MESH = pl.DeviceIdType.MESH
F32 = jnp.float32
BF16 = jnp.bfloat16

RING, TREE, FLAT = (1, 1, 1, 1), (1, 1, 1, 2), (1, 2, 1, 2)
RS_HOPS = (TREE, TREE, TREE, FLAT)
AG_HOPS = (RING, FLAT)


def kernel(
    x_hbm, gate_hbm, up_hbm, hid_hbm, w_hbm,
    dx_ref, dw_ref,
    gate_v, up_v, hid_v, w_v, x_v, g_all, x_all, x_mat, part, ring, fin, landed,
    load_sem, xs, xr, ps, pr, gs, gr, ags, agr, rss, rsr, fs, fr, turn_sem,
):
    p, t, y = lax.axis_index("pp"), lax.axis_index("tp"), lax.axis_index("dp")
    n_pp, n_dp = lax.axis_size("pp"), lax.axis_size("dp")
    z, xl = t // 2, lax.rem(t, 2)
    core = lax.rem(p, 2)
    nz = 8
    hidden = gate_hbm.shape[0]
    half = g_all.shape[2]
    rest = hidden - half
    cols = w_hbm.shape[1]
    hc = cols // 2

    def zmod(v):
        return lax.rem(v + 2 * nz, nz)

    def ymod(v):
        return lax.rem(v + 2 * n_dp, n_dp)

    def at_z(d):
        return (p, zmod(z + d) * 2 + xl, y)

    def at_y(d):
        return (p, t, ymod(y + d))

    partner = (p, t + 1 - 2 * xl, y)

    def remote(src, dst, ssem, rsem, dev):
        return pltpu.make_async_remote_copy(
            src_ref=src, dst_ref=dst, send_sem=ssem, recv_sem=rsem,
            device_id=dev, device_id_type=MESH,
        )

    loads = [
        pltpu.make_async_copy(gate_hbm, gate_v, load_sem.at[0]),
        pltpu.make_async_copy(up_hbm, up_v, load_sem.at[1]),
        pltpu.make_async_copy(hid_hbm, hid_v, load_sem.at[2]),
        pltpu.make_async_copy(w_hbm, w_v, load_sem.at[3]),
        pltpu.make_async_copy(
            x_hbm.at[:, pl.ds(pl.multiple_of(y * cols, 128), cols)],
            x_all.at[z, xl, 0], load_sem.at[4]),
        pltpu.make_async_copy(x_hbm, x_v, load_sem.at[5]),
    ]
    for i in (5, 0, 1, 2, 4, 3):
        loads[i].start()

    barrier = pltpu.get_barrier_semaphore()
    peers = [at_y(1), at_y(2), at_y(3), at_z(1), at_z(-1), at_z(2), at_z(-2), partner,
             (p + 1 - 2 * core, t, y)]
    for d in peers:
        pl.semaphore_signal(barrier, inc=1, device_id=d, device_id_type=MESH)

    @pl.when(p < n_pp - 1)
    def _():
        for j in range(4):
            for xq in range(2):
                pl.semaphore_signal(
                    barrier, inc=1, device_id=(p + 1, z * 2 + xq, j), device_id_type=MESH)

    pl.semaphore_wait(barrier, jnp.where(p > 0, len(peers) + 8, len(peers)))

    sends = []

    def go(c):
        c.start()
        sends.append(c)

    def x_copy(k):
        j = ymod(y + k)
        return remote(
            x_v.at[:, pl.ds(pl.multiple_of(j * cols, 128), cols)],
            x_all.at[z, xl, {1: 2, 2: 3, 3: 1}[k]], xs.at[k - 1], xr.at[k - 1], at_y(k))

    loads[5].wait()
    for k in (2, 1, 3):
        go(x_copy(k))

    for c in loads[:3]:
        c.wait()
    for h, (lo, n) in enumerate(((0, half), (half, rest))):
        rows = pl.ds(lo, n)
        g = gate_v[rows, :].astype(F32)
        u = up_v[rows, :].astype(F32)
        d = hid_v[rows, :].astype(F32)
        s = jax.nn.sigmoid(g)
        v = d * u * s * (1.0 + g * (1.0 - s))
        if n < half:
            v = jnp.concatenate([v, jnp.zeros((half - n, v.shape[1]), F32)], axis=0)
        g_all[0, h] = v.astype(BF16)

    def g_copy(plus, k):
        i, sign = (0, 1) if plus else (1, -1)
        near = 2 if plus else 1
        src, dst, h = ((0, near, i), (0, near, 1 - i), (near, 3, i))[k]
        return remote(
            g_all.at[src, h], g_all.at[dst, h], gs.at[i, k], gr.at[i, k], at_y(sign))

    def g_start():
        for k in (0, 1):
            g_copy(True, k).start()
            g_copy(False, k).start()

    def g_sent():
        for k in (0, 1):
            g_copy(True, k).wait_send()
            g_copy(False, k).wait_send()

    def g_wait(k):
        g_copy(True, k).wait_recv()
        g_copy(False, k).wait_recv()

    def g_forward(plus):
        g_copy(plus, 0).wait_recv()
        go(g_copy(plus, 2))

    def x_wait():
        for k in (1, 3, 2):
            x_copy(k).wait_recv()

    @pl.when(core == 0)
    def _():
        g_start()

    def g_pass():
        g_sent()
        pl.semaphore_signal(turn_sem, inc=1, device_id=(p + 1, t, y), device_id_type=MESH)

    def g_turn():
        pl.semaphore_wait(turn_sem, 1)
        g_start()

    def turn():
        @pl.when(core == 0)
        def _():
            g_pass()

        @pl.when(core == 1)
        def _():
            g_turn()

    def rep(ri):
        return ymod(y + (0, 1, 3, 2)[ri])

    def product(ri):
        g = jnp.concatenate([g_all[ri, 0], g_all[ri, 1]], axis=0)[:hidden]
        for q in range(2):
            c = pl.ds(q * hc, hc)
            acc = lax.dot_general(
                g, w_v[:, c], (((0,), (0,)), ((), ())), preferred_element_type=F32)
            part[ri, :, :, c] = acc.astype(BF16).reshape(nz, 16, hc)

    def lanes(plus, m):
        if m < 4:
            return pl.ds(0, cols)
        return pl.ds(0, hc) if plus else pl.ds(hc, hc)

    def rs_copy(plus, ri, m):
        i, sign = (0, 1) if plus else (1, -1)
        c = lanes(plus, m)
        return remote(
            part.at[ri, zmod(z + sign * m), :, c], ring.at[i, ri, m - 1, :, c],
            rss.at[i, ri, m - 1], rsr.at[i, ri, m - 1], at_z(sign * RS_HOPS[ri][m - 1]))

    def feeds(ri, m):
        return [n for n in range(4, m, -1) if n - RS_HOPS[ri][n - 1] == m]

    def rs_send(ri, m):
        for plus in (True, False):
            i, sign = (0, 1) if plus else (1, -1)
            came = feeds(ri, m)
            for n in came:
                rs_copy(plus, ri, n).wait_recv()
            d = zmod(z + sign * m)
            for q in range(2 if came else 0):
                c = pl.ds(q * hc, hc)
                ms = [n for n in came if n < 4 or plus == (q == 0)]
                if ms:
                    v = part[ri, d, :, c].astype(F32)
                    for n in ms:
                        v = v + ring[i, ri, n - 1, :, c].astype(F32)
                    part[ri, d, :, c] = v.astype(BF16)
            go(rs_copy(plus, ri, m))

    def fin_copy(ri, xq):
        return remote(
            fin.at[ri, xq], landed.at[y, xl], fs.at[ri, xq], fr.at[y, xl],
            (jnp.maximum(p - 1, 0), z * 2 + xq, rep(ri)))

    def rs_end(ri):
        v = part[ri, z].astype(F32)
        for m in feeds(ri, 0):
            for plus in (True, False):
                rs_copy(plus, ri, m).wait_recv()
                v = v + ring[0 if plus else 1, ri, m - 1].astype(F32)
        v = v.reshape(2, 8, cols).astype(BF16)
        for xq in range(2):
            fin[ri, xq] = v[xq]

        @pl.when(p > 0)
        def _():
            for xq in range(2):
                fin_copy(ri, xq).start()

    def pair_send(k):
        go(pair_copy(k))

    def pair_copy(k):
        ref = x_all.at[zmod(z + k), xl]
        return remote(ref, ref, ps.at[k % nz], pr.at[k % nz], partner)

    def ag_copies(g, k):
        out = []
        for plus in (True, False):
            i, sign = (0, 1) if plus else (1, -1)
            lo, n = ((0, 1), (1, 3))[g]
            if k == 4:
                lo, n = (((0, 1), (1, 1)) if plus else ((0, 0), (2, 2)))[g]
            if n == 0:
                continue
            hop = AG_HOPS[g][k - 1]
            ref = x_all.at[zmod(z - sign * (k - hop)), xl, pl.ds(lo, n)]
            out.append(remote(
                ref, ref, ags.at[g, i, k - 1], agr.at[g, i, k - 1], at_z(sign * hop)))
        return out

    def ag_send(g, k):
        for c in ag_copies(g, k):
            go(c)

    def ag_wait(g, k):
        for c in ag_copies(g, k):
            c.wait_recv()

    loads[4].wait()
    loads[3].wait()
    product(0)
    rs_send(0, 3)
    rs_send(0, 4)
    ag_send(0, 1)
    x_wait()
    ag_send(1, 2)
    ag_wait(0, 1)
    ag_send(0, 2)
    turn()
    pair_send(0)
    ag_send(1, 1)
    g_forward(False)
    g_forward(True)
    rs_send(0, 2)
    g_wait(1)
    product(1)
    rs_send(1, 4)
    product(2)
    rs_send(2, 3)
    rs_send(1, 3)
    rs_send(2, 4)
    ag_wait(0, 2)
    ag_wait(1, 2)
    pair_send(2)
    pair_send(-2)
    ag_send(1, 3)
    ag_send(0, 3)
    ag_send(1, 4)
    g_wait(2)
    product(3)
    rs_send(3, 4)
    ag_wait(1, 1)
    pair_send(1)
    pair_send(-1)
    rs_send(1, 2)
    rs_send(3, 3)
    rs_send(2, 2)
    rs_send(3, 1)
    ag_wait(0, 3)
    ag_wait(1, 3)
    pair_send(3)
    pair_send(-3)
    ag_send(0, 4)
    rs_send(0, 1)
    rs_send(1, 1)
    rs_send(3, 2)
    rs_send(2, 1)
    ag_wait(0, 4)
    ag_wait(1, 4)
    pair_send(4)
    rs_end(0)
    rs_end(1)
    rs_end(2)
    rs_end(3)

    for k in range(nz):
        pair_copy(k).wait_recv()
    for r in range(4):
        x_mat[pl.ds(r * 128, 128), :] = (
            x_all[:, :, r].astype(F32).reshape(128, cols).astype(BF16))
    for lo in range(0, hidden, 128):
        n = min(128, hidden - lo)
        pieces = []
        for r in range(4):
            if lo + n <= half:
                pieces.append(g_all[r, 0, pl.ds(lo, n), :])
            elif lo >= half:
                pieces.append(g_all[r, 1, pl.ds(lo - half, n), :])
            else:
                pieces.append(jnp.concatenate(
                    [g_all[r, 0, pl.ds(lo, half - lo), :],
                     g_all[r, 1, pl.ds(0, lo + n - half), :]], axis=0))
        g = jnp.concatenate(pieces, axis=1)
        dw_ref[pl.ds(lo, n), :] = jnp.dot(
            g, x_mat[...], preferred_element_type=F32).astype(BF16)

    @pl.when(p < n_pp - 1)
    def _():
        for j in range(4):
            for xq in range(2):
                remote(
                    landed.at[j, xq], landed.at[j, xq], fs.at[0, 0], fr.at[j, xq],
                    partner).wait_recv()
            dx_ref[:, pl.ds(j * cols, cols)] = (
                landed[j, 0].astype(F32) + landed[j, 1].astype(F32)).astype(BF16)

    @pl.when(p == n_pp - 1)
    def _():
        dx_ref[...] = jnp.zeros_like(dx_ref)

    for c in sends:
        c.wait_send()

    @pl.when(core == 1)
    def _():
        g_sent()


    @pl.when(p > 0)
    def _():
        for ri in range(4):
            for xq in range(2):
                fin_copy(ri, xq).wait_send()


def on_device(layer_input, gate_pre, up_pre, hidden_grad, gate_weight):
    x = layer_input[0, 0]
    gate, up, hid = (jnp.swapaxes(v[0, 0], 0, 1) for v in (gate_pre, up_pre, hidden_grad))
    w = jnp.swapaxes(gate_weight[0], 0, 1)
    hidden, toks = gate.shape
    cols = w.shape[1]
    half = (hidden // 2 + 15) // 16 * 16
    vm = pltpu.VMEM
    dma = pltpu.SemaphoreType.DMA
    dx, dw = pl.pallas_call(
        kernel,
        name="section",
        out_shape=(
            jax.ShapeDtypeStruct(x.shape, BF16),
            jax.ShapeDtypeStruct((hidden, cols), BF16),
        ),
        in_specs=[pl.BlockSpec(memory_space=pltpu.HBM)] * 5,
        out_specs=[pl.BlockSpec(memory_space=pltpu.VMEM)] * 2,
        scratch_shapes=[
            vm((hidden, toks), BF16), vm((hidden, toks), BF16), vm((hidden, toks), BF16),
            vm((hidden, cols), BF16),
            vm(x.shape, BF16),
            vm((4, 2, half, toks), BF16),
            vm((8, 2, 4, 8, cols), BF16),
            vm((512, cols), BF16),
            vm((4, 8, 16, cols), BF16),
            vm((2, 4, 4, 16, cols), BF16),
            vm((4, 2, 8, cols), BF16),
            vm((4, 2, 8, cols), BF16),
            dma((6,)), dma((3,)), dma((3,)), dma((8,)), dma((8,)),
            dma((2, 3)), dma((2, 3)),
            dma((2, 2, 4)), dma((2, 2, 4)),
            dma((2, 4, 4)), dma((2, 4, 4)),
            dma((4, 2)), dma((4, 2)), pltpu.SemaphoreType.REGULAR,
        ],
        compiler_params=pltpu.CompilerParams(
            collective_id=0, has_side_effects=True, vmem_limit_bytes=40 << 20),
    )(*(pltpu.with_memory_space_constraint(v, pltpu.HBM) for v in (x, gate, up, hid, w)))
    return dx[None, None], jnp.swapaxes(dw, 0, 1)[None]


def solution(mesh):
    return jax.shard_map(
        on_device,
        mesh=mesh,
        in_specs=(
            P("pp", "dp", "tp", None),
            P("pp", "dp", None, "tp"),
            P("pp", "dp", None, "tp"),
            P("pp", "dp", None, "tp"),
            P("pp", "dp", "tp"),
        ),
        out_specs=(P("pp", "dp", "tp", None), P("pp", "dp", "tp")),
        check_vma=False,
    )
```

```python
import jax
import jax.numpy as jnp
from jax import lax
from jax.experimental import pallas as pl
from jax.experimental.pallas import tpu as pltpu
from jax.sharding import PartitionSpec as P

MESH = pl.DeviceIdType.MESH
F32 = jnp.float32
BF16 = jnp.bfloat16

RING, TREE, FLAT = (1, 1, 1, 1), (1, 1, 1, 2), (1, 2, 1, 2)
RS_HOPS = (
    (FLAT, FLAT, TREE, FLAT),
    (FLAT, TREE, RING, FLAT),
)
AG_HOPS = ((FLAT, FLAT), (TREE, TREE))


def kernel(
    x_hbm, gate_hbm, up_hbm, hid_hbm, w_hbm,
    dx_ref, dw_ref,
    gate_v, up_v, hid_v, w_v, x_v, g_all, x_all, x_mat, part, ring, fin, landed,
    load_sem, xs, xr, ps, pr, gs, gr, ags, agr, rss, rsr, fs, fr, turn_sem,
):
    p, t, y = lax.axis_index("pp"), lax.axis_index("tp"), lax.axis_index("dp")
    n_pp, n_dp = lax.axis_size("pp"), lax.axis_size("dp")
    z, xl = t // 2, lax.rem(t, 2)
    core = lax.rem(p, 2)
    nz = 8
    hidden = gate_hbm.shape[0]
    half = g_all.shape[2]
    rest = hidden - half
    cols = w_hbm.shape[1]
    hc = cols // 2

    def zmod(v):
        return lax.rem(v + 2 * nz, nz)

    def ymod(v):
        return lax.rem(v + 2 * n_dp, n_dp)

    def at_z(d):
        return (p, zmod(z + d) * 2 + xl, y)

    def at_y(d):
        return (p, t, ymod(y + d))

    partner = (p, t + 1 - 2 * xl, y)

    def remote(src, dst, ssem, rsem, dev):
        return pltpu.make_async_remote_copy(
            src_ref=src, dst_ref=dst, send_sem=ssem, recv_sem=rsem,
            device_id=dev, device_id_type=MESH,
        )

    loads = [
        pltpu.make_async_copy(gate_hbm, gate_v, load_sem.at[0]),
        pltpu.make_async_copy(up_hbm, up_v, load_sem.at[1]),
        pltpu.make_async_copy(hid_hbm, hid_v, load_sem.at[2]),
        pltpu.make_async_copy(w_hbm, w_v, load_sem.at[3]),
        pltpu.make_async_copy(
            x_hbm.at[:, pl.ds(pl.multiple_of(y * cols, 128), cols)],
            x_all.at[z, xl, 0], load_sem.at[4]),
        pltpu.make_async_copy(x_hbm, x_v, load_sem.at[5]),
    ]
    for i in (5, 0, 1, 2, 4, 3):
        loads[i].start()

    barrier = pltpu.get_barrier_semaphore()
    peers = [at_y(1), at_y(2), at_y(3), at_z(1), at_z(-1), at_z(2), at_z(-2), partner,
             (p + 1 - 2 * core, t, y)]
    for d in peers:
        pl.semaphore_signal(barrier, inc=1, device_id=d, device_id_type=MESH)

    @pl.when(p < n_pp - 1)
    def _():
        for j in range(4):
            for xq in range(2):
                pl.semaphore_signal(
                    barrier, inc=1, device_id=(p + 1, z * 2 + xq, j), device_id_type=MESH)

    pl.semaphore_wait(barrier, jnp.where(p > 0, len(peers) + 8, len(peers)))

    side = [0]

    def go(c):
        c.start()

    def x_copy(k):
        j = ymod(y + k)
        return remote(
            x_v.at[:, pl.ds(pl.multiple_of(j * cols, 128), cols)],
            x_all.at[z, xl, {1: 2, 2: 3, 3: 1}[k]], xs.at[k - 1], xr.at[k - 1], at_y(k))

    loads[5].wait()
    for k in (2, 1, 3):
        go(x_copy(k))

    for c in loads[:3]:
        c.wait()
    for h, (lo, n) in enumerate(((0, half), (half, rest))):
        rows = pl.ds(lo, n)
        g = gate_v[rows, :].astype(F32)
        u = up_v[rows, :].astype(F32)
        d = hid_v[rows, :].astype(F32)
        s = jax.nn.sigmoid(g)
        v = d * u * s * (1.0 + g * (1.0 - s))
        if n < half:
            v = jnp.concatenate([v, jnp.zeros((half - n, v.shape[1]), F32)], axis=0)
        g_all[0, h] = v.astype(BF16)

    def g_copy(plus, k):
        i, sign = (0, 1) if plus else (1, -1)
        near = 2 if plus else 1
        src, dst, h = ((0, near, i), (0, near, 1 - i), (near, 3, i))[k]
        return remote(
            g_all.at[src, h], g_all.at[dst, h], gs.at[i, k], gr.at[i, k], at_y(sign))

    def g_start():
        for k in (0, 1):
            g_copy(True, k).start()
            g_copy(False, k).start()

    def g_sent(*ks):
        for k in ks:
            g_copy(True, k).wait_send()
            g_copy(False, k).wait_send()

    def g_recv(plus, k):
        g_copy(plus, k).wait_recv()

    def g_forward(plus):
        go(g_copy(plus, 2))

    def x_wait():
        for k in (1, 3, 2):
            x_copy(k).wait_recv()

    @pl.when(core == 0)
    def _():
        g_start()

    def g_pass():
        g_sent(0)
        pl.semaphore_signal(turn_sem, inc=1, device_id=(p + 1, t, y), device_id_type=MESH)

    def g_turn():
        pl.semaphore_wait(turn_sem, 1)
        g_start()

    def rep(ri):
        return ymod(y + (0, 1, 3, 2)[ri])

    def product(ri):
        g = jnp.concatenate([g_all[ri, 0], g_all[ri, 1]], axis=0)[:hidden]
        for q in range(2):
            c = pl.ds(q * hc, hc)
            acc = lax.dot_general(
                g, w_v[:, c], (((0,), (0,)), ((), ())), preferred_element_type=F32)
            part[ri, :, :, c] = acc.astype(BF16).reshape(nz, 16, hc)

    def lanes(plus, m):
        if m < 4:
            return pl.ds(0, cols)
        return pl.ds(0, hc) if plus else pl.ds(hc, hc)

    def rs_copy(plus, ri, m):
        i, sign = (0, 1) if plus else (1, -1)
        c = lanes(plus, m)
        return remote(
            part.at[ri, zmod(z + sign * m), :, c], ring.at[i, ri, m - 1, :, c],
            rss.at[i, ri, m - 1], rsr.at[i, ri, m - 1], at_z(sign * RS_HOPS[side[0]][ri][m - 1]))

    def feeds(ri, m):
        return [n for n in range(4, m, -1) if n - RS_HOPS[side[0]][ri][n - 1] == m]

    def rs_send(ri, m):
        for plus in (True, False):
            i, sign = (0, 1) if plus else (1, -1)
            came = feeds(ri, m)
            for n in came:
                rs_copy(plus, ri, n).wait_recv()
            d = zmod(z + sign * m)
            for q in range(2 if came else 0):
                c = pl.ds(q * hc, hc)
                ms = [n for n in came if n < 4 or plus == (q == 0)]
                if ms:
                    v = part[ri, d, :, c].astype(F32)
                    for n in ms:
                        v = v + ring[i, ri, n - 1, :, c].astype(F32)
                    part[ri, d, :, c] = v.astype(BF16)
            go(rs_copy(plus, ri, m))

    def fin_copy(ri, xq):
        return remote(
            fin.at[ri, xq], landed.at[y, xl], fs.at[ri, xq], fr.at[y, xl],
            (jnp.maximum(p - 1, 0), z * 2 + xq, rep(ri)))

    def rs_end(ri):
        v = part[ri, z].astype(F32)
        for m in feeds(ri, 0):
            for plus in (True, False):
                rs_copy(plus, ri, m).wait_recv()
                v = v + ring[0 if plus else 1, ri, m - 1].astype(F32)
        v = v.reshape(2, 8, cols).astype(BF16)
        for xq in range(2):
            fin[ri, xq] = v[xq]

        @pl.when(p > 0)
        def _():
            for xq in range(2):
                fin_copy(ri, xq).start()

    def pair_send(k):
        go(pair_copy(k))

    def pair_copy(k):
        ref = x_all.at[zmod(z + k), xl]
        return remote(ref, ref, ps.at[k % nz], pr.at[k % nz], partner)

    def ag_copies(g, k):
        out = []
        for plus in (True, False):
            i, sign = (0, 1) if plus else (1, -1)
            lo, n = ((0, 1), (1, 3))[g]
            if k == 4:
                lo, n = (((0, 1), (1, 1)) if plus else ((0, 0), (2, 2)))[g]
            if n == 0:
                continue
            hop = AG_HOPS[side[0]][g][k - 1]
            ref = x_all.at[zmod(z - sign * (k - hop)), xl, pl.ds(lo, n)]
            out.append(remote(
                ref, ref, ags.at[g, i, k - 1], agr.at[g, i, k - 1], at_z(sign * hop)))
        return out

    def ag_send(g, k):
        for c in ag_copies(g, k):
            go(c)

    def ag_wait(g, k):
        for c in ag_copies(g, k):
            c.wait_recv()

    loads[4].wait()

    @pl.when(core == 0)
    def _():
        side[0] = 0
        loads[3].wait()
        product(0)
        rs_send(0, 3)
        rs_send(0, 4)
        rs_send(0, 1)
        ag_send(0, 2)
        g_pass()
        ag_send(0, 1)
        x_wait()
        ag_send(1, 2)
        rs_send(0, 2)
        ag_wait(0, 2)
        ag_send(0, 4)
        g_recv(True, 0)
        g_forward(True)
        g_recv(False, 0)
        g_forward(False)
        ag_send(1, 1)
        g_recv(False, 1)
        product(1)
        g_recv(True, 1)
        product(2)
        rs_send(1, 4)
        rs_send(2, 4)
        rs_send(2, 3)
        rs_send(1, 3)
        ag_wait(1, 2)
        ag_send(1, 4)
        pair_send(2)
        pair_send(-2)
        ag_send(1, 3)
        pair_send(0)
        g_recv(True, 2)
        g_recv(False, 2)
        product(3)
        rs_send(3, 4)
        ag_send(0, 3)
        rs_send(3, 3)
        rs_end(0)
        rs_send(2, 2)
        rs_send(1, 2)
        ag_wait(0, 4)
        ag_wait(1, 4)
        pair_send(4)
        ag_wait(0, 1)
        ag_wait(1, 1)
        pair_send(1)
        pair_send(-1)
        rs_send(1, 1)
        rs_send(3, 2)
        rs_send(3, 1)
        ag_wait(0, 3)
        ag_wait(1, 3)
        pair_send(3)
        pair_send(-3)
        rs_send(2, 1)
        rs_end(3)
        rs_end(1)
        rs_end(2)

    @pl.when(core == 1)
    def _():
        side[0] = 1
        ag_send(0, 1)
        loads[3].wait()
        product(0)
        rs_send(0, 1)
        rs_send(0, 4)
        ag_wait(0, 1)
        ag_send(0, 2)
        rs_send(0, 3)
        x_wait()
        ag_send(1, 1)
        g_turn()
        rs_send(0, 2)
        g_recv(False, 0)
        g_recv(False, 1)
        product(1)
        g_recv(True, 0)
        g_recv(True, 1)
        product(2)
        ag_wait(1, 1)
        ag_send(1, 2)
        rs_send(2, 4)
        pair_send(1)
        pair_send(-1)
        g_forward(False)
        rs_send(1, 3)
        g_forward(True)
        g_recv(True, 2)
        g_recv(False, 2)
        product(3)
        rs_send(1, 4)
        rs_send(2, 3)
        rs_send(3, 3)
        rs_send(3, 4)
        rs_send(1, 2)
        ag_wait(0, 2)
        ag_send(0, 3)
        ag_wait(1, 2)
        pair_send(2)
        pair_send(-2)
        pair_send(0)
        ag_send(1, 3)
        rs_send(2, 2)
        ag_send(1, 4)
        ag_send(0, 4)
        rs_send(3, 2)
        rs_send(3, 1)
        rs_end(0)
        rs_send(1, 1)
        ag_wait(0, 3)
        ag_wait(1, 3)
        pair_send(3)
        pair_send(-3)
        rs_send(2, 1)
        ag_wait(0, 4)
        ag_wait(1, 4)
        pair_send(4)
        rs_end(3)
        rs_end(1)
        rs_end(2)

    side[0] = 0

    for k in range(nz):
        pair_copy(k).wait_recv()
    for r in range(4):
        x_mat[pl.ds(r * 128, 128), :] = (
            x_all[:, :, r].astype(F32).reshape(128, cols).astype(BF16))
    for lo in range(0, hidden, 128):
        n = min(128, hidden - lo)
        pieces = []
        for r in range(4):
            if lo + n <= half:
                pieces.append(g_all[r, 0, pl.ds(lo, n), :])
            elif lo >= half:
                pieces.append(g_all[r, 1, pl.ds(lo - half, n), :])
            else:
                pieces.append(jnp.concatenate(
                    [g_all[r, 0, pl.ds(lo, half - lo), :],
                     g_all[r, 1, pl.ds(0, lo + n - half), :]], axis=0))
        g = jnp.concatenate(pieces, axis=1)
        dw_ref[pl.ds(lo, n), :] = jnp.dot(
            g, x_mat[...], preferred_element_type=F32).astype(BF16)

    @pl.when(p < n_pp - 1)
    def _():
        for j in range(4):
            for xq in range(2):
                remote(
                    landed.at[j, xq], landed.at[j, xq], fs.at[0, 0], fr.at[j, xq],
                    partner).wait_recv()
            dx_ref[:, pl.ds(j * cols, cols)] = (
                landed[j, 0].astype(F32) + landed[j, 1].astype(F32)).astype(BF16)

    @pl.when(p == n_pp - 1)
    def _():
        dx_ref[...] = jnp.zeros_like(dx_ref)

    for k in (1, 2, 3):
        x_copy(k).wait_send()
    for k in range(nz):
        pair_copy(k).wait_send()
    for k in range(1, 5):
        for g in range(2):
            for c in ag_copies(g, k):
                c.wait_send()
        for plus in (True, False):
            for ri in range(4):
                rs_copy(plus, ri, k).wait_send()
    for plus in (True, False):
        g_copy(plus, 2).wait_send()

    g_sent(1)

    @pl.when(core == 1)
    def _():
        g_sent(0)


    @pl.when(p > 0)
    def _():
        for ri in range(4):
            for xq in range(2):
                fin_copy(ri, xq).wait_send()


def write_out(dx_v, dw_v, dx_hbm, dw_hbm, sem):
    copies = [
        pltpu.make_async_copy(dw_v, dw_hbm, sem.at[0]),
        pltpu.make_async_copy(dx_v, dx_hbm, sem.at[1]),
    ]
    for c in copies:
        c.start()
    for c in copies:
        c.wait()


def on_device(layer_input, gate_pre, up_pre, hidden_grad, gate_weight):
    x = layer_input[0, 0]
    gate, up, hid = (jnp.swapaxes(v[0, 0], 0, 1) for v in (gate_pre, up_pre, hidden_grad))
    w = jnp.swapaxes(gate_weight[0], 0, 1)
    hidden, toks = gate.shape
    cols = w.shape[1]
    half = (hidden // 2 + 15) // 16 * 16
    vm = pltpu.VMEM
    dma = pltpu.SemaphoreType.DMA
    dx, dw = pl.pallas_call(
        kernel,
        name="section",
        out_shape=(
            jax.ShapeDtypeStruct(x.shape, BF16),
            jax.ShapeDtypeStruct((hidden, cols), BF16),
        ),
        in_specs=[pl.BlockSpec(memory_space=pltpu.HBM)] * 5,
        out_specs=[pl.BlockSpec(memory_space=pltpu.VMEM)] * 2,
        scratch_shapes=[
            vm((hidden, toks), BF16), vm((hidden, toks), BF16), vm((hidden, toks), BF16),
            vm((hidden, cols), BF16),
            vm(x.shape, BF16),
            vm((4, 2, half, toks), BF16),
            vm((8, 2, 4, 8, cols), BF16),
            vm((512, cols), BF16),
            vm((4, 8, 16, cols), BF16),
            vm((2, 4, 4, 16, cols), BF16),
            vm((4, 2, 8, cols), BF16),
            vm((4, 2, 8, cols), BF16),
            dma((6,)), dma((3,)), dma((3,)), dma((8,)), dma((8,)),
            dma((2, 3)), dma((2, 3)),
            dma((2, 2, 4)), dma((2, 2, 4)),
            dma((2, 4, 4)), dma((2, 4, 4)),
            dma((4, 2)), dma((4, 2)), pltpu.SemaphoreType.REGULAR,
        ],
        compiler_params=pltpu.CompilerParams(
            collective_id=0, has_side_effects=True, vmem_limit_bytes=40 << 20),
    )(*(pltpu.with_memory_space_constraint(v, pltpu.HBM) for v in (x, gate, up, hid, w)))
    dx, dw = pl.pallas_call(
        write_out,
        name="write_out",
        out_shape=(
            jax.ShapeDtypeStruct(x.shape, BF16),
            jax.ShapeDtypeStruct((hidden, cols), BF16),
        ),
        in_specs=[pl.BlockSpec(memory_space=pltpu.VMEM)] * 2,
        out_specs=[pl.BlockSpec(memory_space=pltpu.HBM)] * 2,
        scratch_shapes=[dma((2,))],
        compiler_params=pltpu.CompilerParams(vmem_limit_bytes=8 << 20),
    )(dx, dw)
    return dx[None, None], jnp.swapaxes(dw, 0, 1)[None]


def solution(mesh):
    return jax.shard_map(
        on_device,
        mesh=mesh,
        in_specs=(
            P("pp", "dp", "tp", None),
            P("pp", "dp", None, "tp"),
            P("pp", "dp", None, "tp"),
            P("pp", "dp", None, "tp"),
            P("pp", "dp", "tp"),
        ),
        out_specs=(P("pp", "dp", "tp", None), P("pp", "dp", "tp")),
        check_vma=False,
    )
```

```python
import jax
import jax.numpy as jnp
from jax import lax
from jax.experimental import pallas as pl
from jax.experimental.pallas import tpu as pltpu
from jax.sharding import PartitionSpec as P

MESH = pl.DeviceIdType.MESH
F32 = jnp.float32
BF16 = jnp.bfloat16

RING, TREE, FLAT = (1, 1, 1, 1), (1, 1, 1, 2), (1, 2, 1, 2)
RS_HOPS = (
    (FLAT, FLAT, TREE, FLAT),
    (FLAT, TREE, RING, FLAT),
)
AG_HOPS = ((FLAT, FLAT), (TREE, TREE))


def kernel(
    x_hbm, gate_hbm, up_hbm, hid_hbm, w_hbm,
    dx_ref, dw_ref,
    gate_v, up_v, hid_v, w_v, x_v, g_all, x_all, x_mat, part, ring, fin, landed,
    load_sem, xs, xr, ps, pr, gs, gr, ags, agr, rss, rsr, fs, fr, turn_sem,
):
    p, t, y = lax.axis_index("pp"), lax.axis_index("tp"), lax.axis_index("dp")
    n_pp, n_dp = lax.axis_size("pp"), lax.axis_size("dp")
    z, xl = t // 2, lax.rem(t, 2)
    core = lax.rem(p, 2)
    nz = 8
    hidden = gate_hbm.shape[0]
    half = g_all.shape[2]
    rest = hidden - half
    cols = w_hbm.shape[1]
    hc = cols // 2

    def zmod(v):
        return lax.rem(v + 2 * nz, nz)

    def ymod(v):
        return lax.rem(v + 2 * n_dp, n_dp)

    def at_z(d):
        return (p, zmod(z + d) * 2 + xl, y)

    def at_y(d):
        return (p, t, ymod(y + d))

    partner = (p, t + 1 - 2 * xl, y)

    def remote(src, dst, ssem, rsem, dev):
        return pltpu.make_async_remote_copy(
            src_ref=src, dst_ref=dst, send_sem=ssem, recv_sem=rsem,
            device_id=dev, device_id_type=MESH,
        )

    loads = [
        pltpu.make_async_copy(gate_hbm, gate_v, load_sem.at[0]),
        pltpu.make_async_copy(up_hbm, up_v, load_sem.at[1]),
        pltpu.make_async_copy(hid_hbm, hid_v, load_sem.at[2]),
        pltpu.make_async_copy(w_hbm, w_v, load_sem.at[3]),
        pltpu.make_async_copy(
            x_hbm.at[:, pl.ds(pl.multiple_of(y * cols, 128), cols)],
            x_all.at[z, xl, 0], load_sem.at[4]),
        pltpu.make_async_copy(x_hbm, x_v, load_sem.at[5]),
    ]
    for i in (5, 0, 1, 2, 4, 3):
        loads[i].start()

    barrier = pltpu.get_barrier_semaphore()
    peers = [at_y(1), at_y(2), at_y(3), at_z(1), at_z(-1), at_z(2), at_z(-2), partner,
             (p + 1 - 2 * core, t, y)]
    for d in peers:
        pl.semaphore_signal(barrier, inc=1, device_id=d, device_id_type=MESH)

    @pl.when(p < n_pp - 1)
    def _():
        for j in range(4):
            for xq in range(2):
                pl.semaphore_signal(
                    barrier, inc=1, device_id=(p + 1, z * 2 + xq, j), device_id_type=MESH)

    pl.semaphore_wait(barrier, jnp.where(p > 0, len(peers) + 8, len(peers)))

    side = [0]

    def go(c):
        c.start()

    def x_copy(k):
        j = ymod(y + k)
        return remote(
            x_v.at[:, pl.ds(pl.multiple_of(j * cols, 128), cols)],
            x_all.at[z, xl, {1: 2, 2: 3, 3: 1}[k]], xs.at[k - 1], xr.at[k - 1], at_y(k))

    loads[5].wait()
    for k in (2, 1, 3):
        go(x_copy(k))

    for c in loads[:3]:
        c.wait()
    for h, (lo, n) in enumerate(((0, half), (half, rest))):
        rows = pl.ds(lo, n)
        g = gate_v[rows, :].astype(F32)
        u = up_v[rows, :].astype(F32)
        d = hid_v[rows, :].astype(F32)
        s = jax.nn.sigmoid(g)
        v = d * u * s * (1.0 + g * (1.0 - s))
        if n < half:
            v = jnp.concatenate([v, jnp.zeros((half - n, v.shape[1]), F32)], axis=0)
        g_all[0, h] = v.astype(BF16)

    def g_copy(plus, k):
        i, sign = (0, 1) if plus else (1, -1)
        near = 2 if plus else 1
        src, dst, h = ((0, near, i), (0, near, 1 - i), (near, 3, i))[k]
        return remote(
            g_all.at[src, h], g_all.at[dst, h], gs.at[i, k], gr.at[i, k], at_y(sign))

    def g_start():
        for k in (0, 1):
            g_copy(True, k).start()
            g_copy(False, k).start()

    def g_sent(*ks):
        for k in ks:
            g_copy(True, k).wait_send()
            g_copy(False, k).wait_send()

    def g_recv(plus, k):
        g_copy(plus, k).wait_recv()

    def g_forward(plus):
        go(g_copy(plus, 2))

    def x_wait():
        for k in (1, 3, 2):
            x_copy(k).wait_recv()

    @pl.when(core == 0)
    def _():
        g_start()

    def g_pass():
        g_sent(0)
        pl.semaphore_signal(turn_sem, inc=1, device_id=(p + 1, t, y), device_id_type=MESH)

    def g_turn():
        pl.semaphore_wait(turn_sem, 1)
        g_start()

    def rep(ri):
        return ymod(y + (0, 1, 3, 2)[ri])

    def product(ri):
        g = jnp.concatenate([g_all[ri, 0], g_all[ri, 1]], axis=0)[:hidden]
        for q in range(2):
            c = pl.ds(q * hc, hc)
            acc = lax.dot_general(
                g, w_v[:, c], (((0,), (0,)), ((), ())), preferred_element_type=F32)
            part[ri, :, :, c] = acc.astype(BF16).reshape(nz, 16, hc)

    def lanes(plus, m):
        if m < 4:
            return pl.ds(0, cols)
        return pl.ds(0, hc) if plus else pl.ds(hc, hc)

    def rs_copy(plus, ri, m):
        i, sign = (0, 1) if plus else (1, -1)
        c = lanes(plus, m)
        return remote(
            part.at[ri, zmod(z + sign * m), :, c], ring.at[i, ri, m - 1, :, c],
            rss.at[i, ri, m - 1], rsr.at[i, ri, m - 1], at_z(sign * RS_HOPS[side[0]][ri][m - 1]))

    def feeds(ri, m):
        return [n for n in range(4, m, -1) if n - RS_HOPS[side[0]][ri][n - 1] == m]

    def rs_send(ri, m):
        for plus in (True, False):
            i, sign = (0, 1) if plus else (1, -1)
            came = feeds(ri, m)
            for n in came:
                rs_copy(plus, ri, n).wait_recv()
            d = zmod(z + sign * m)
            for q in range(2 if came else 0):
                c = pl.ds(q * hc, hc)
                ms = [n for n in came if n < 4 or plus == (q == 0)]
                if ms:
                    v = part[ri, d, :, c].astype(F32)
                    for n in ms:
                        v = v + ring[i, ri, n - 1, :, c].astype(F32)
                    part[ri, d, :, c] = v.astype(BF16)
            go(rs_copy(plus, ri, m))

    def fin_copy(ri, xq):
        return remote(
            fin.at[ri, xq], landed.at[y, xl], fs.at[ri, xq], fr.at[y, xl],
            (jnp.maximum(p - 1, 0), z * 2 + xq, rep(ri)))

    def rs_end(ri):
        v = part[ri, z].astype(F32)
        for m in feeds(ri, 0):
            for plus in (True, False):
                rs_copy(plus, ri, m).wait_recv()
                v = v + ring[0 if plus else 1, ri, m - 1].astype(F32)
        v = v.reshape(2, 8, cols).astype(BF16)
        for xq in range(2):
            fin[ri, xq] = v[xq]

        @pl.when(p > 0)
        def _():
            for xq in range(2):
                fin_copy(ri, xq).start()

    def pair_send(k):
        go(pair_copy(k))

    def pair_copy(k):
        ref = x_all.at[zmod(z + k), xl]
        return remote(ref, ref, ps.at[k % nz], pr.at[k % nz], partner)

    def ag_copies(g, k):
        out = []
        for plus in (True, False):
            i, sign = (0, 1) if plus else (1, -1)
            lo, n = ((0, 1), (1, 3))[g]
            if k == 4:
                lo, n = (((0, 1), (1, 1)) if plus else ((0, 0), (2, 2)))[g]
            if n == 0:
                continue
            hop = AG_HOPS[side[0]][g][k - 1]
            ref = x_all.at[zmod(z - sign * (k - hop)), xl, pl.ds(lo, n)]
            out.append(remote(
                ref, ref, ags.at[g, i, k - 1], agr.at[g, i, k - 1], at_z(sign * hop)))
        return out

    def ag_send(g, k):
        for c in ag_copies(g, k):
            go(c)

    def ag_wait(g, k):
        for c in ag_copies(g, k):
            c.wait_recv()

    loads[4].wait()

    @pl.when(core == 0)
    def _():
        side[0] = 0
        loads[3].wait()
        product(0)
        rs_send(0, 3)
        rs_send(0, 4)
        rs_send(0, 1)
        ag_send(0, 2)
        g_pass()
        ag_send(0, 1)
        x_wait()
        ag_send(1, 2)
        g_recv(True, 0)
        g_forward(True)
        g_recv(False, 0)
        g_forward(False)
        rs_send(0, 2)
        ag_wait(0, 2)
        ag_send(0, 4)
        ag_send(1, 1)
        g_recv(False, 1)
        product(1)
        g_recv(True, 1)
        product(2)
        rs_send(1, 4)
        rs_send(2, 4)
        rs_send(2, 3)
        rs_send(1, 3)
        ag_wait(1, 2)
        ag_send(1, 4)
        pair_send(2)
        pair_send(-2)
        ag_send(1, 3)
        pair_send(0)
        g_recv(True, 2)
        g_recv(False, 2)
        product(3)
        rs_send(3, 4)
        ag_send(0, 3)
        rs_send(3, 3)
        rs_end(0)
        rs_send(2, 2)
        rs_send(1, 2)
        ag_wait(0, 4)
        ag_wait(1, 4)
        pair_send(4)
        ag_wait(0, 1)
        ag_wait(1, 1)
        pair_send(1)
        pair_send(-1)
        rs_send(1, 1)
        rs_send(3, 2)
        rs_send(3, 1)
        ag_wait(0, 3)
        ag_wait(1, 3)
        pair_send(3)
        pair_send(-3)
        rs_send(2, 1)
        rs_end(3)
        rs_end(1)
        rs_end(2)

    @pl.when(core == 1)
    def _():
        side[0] = 1
        ag_send(0, 1)
        loads[3].wait()
        product(0)
        rs_send(0, 1)
        rs_send(0, 4)
        ag_wait(0, 1)
        ag_send(0, 2)
        rs_send(0, 3)
        x_wait()
        ag_send(1, 1)
        pair_send(0)
        g_turn()
        rs_send(0, 2)
        g_recv(True, 0)
        g_forward(True)
        g_recv(False, 0)
        g_forward(False)
        g_recv(False, 1)
        product(1)
        g_recv(True, 1)
        product(2)
        ag_wait(1, 1)
        ag_send(1, 2)
        rs_send(2, 4)
        pair_send(1)
        pair_send(-1)
        rs_send(1, 3)
        g_recv(True, 2)
        g_recv(False, 2)
        product(3)
        rs_send(1, 4)
        rs_send(2, 3)
        rs_send(3, 3)
        rs_send(3, 4)
        ag_wait(0, 2)
        ag_send(0, 3)
        ag_wait(1, 2)
        ag_send(1, 3)
        pair_send(2)
        pair_send(-2)
        rs_send(1, 2)
        rs_send(2, 2)
        ag_send(1, 4)
        ag_send(0, 4)
        rs_send(3, 2)
        rs_send(3, 1)
        rs_end(0)
        rs_send(1, 1)
        ag_wait(0, 3)
        ag_wait(1, 3)
        pair_send(3)
        pair_send(-3)
        rs_send(2, 1)
        ag_wait(0, 4)
        ag_wait(1, 4)
        pair_send(4)
        rs_end(3)
        rs_end(1)
        rs_end(2)

    side[0] = 0

    for k in range(nz):
        pair_copy(k).wait_recv()
    for r in range(4):
        x_mat[pl.ds(r * 128, 128), :] = (
            x_all[:, :, r].astype(F32).reshape(128, cols).astype(BF16))
    for lo in range(0, hidden, 128):
        n = min(128, hidden - lo)
        pieces = []
        for r in range(4):
            if lo + n <= half:
                pieces.append(g_all[r, 0, pl.ds(lo, n), :])
            elif lo >= half:
                pieces.append(g_all[r, 1, pl.ds(lo - half, n), :])
            else:
                pieces.append(jnp.concatenate(
                    [g_all[r, 0, pl.ds(lo, half - lo), :],
                     g_all[r, 1, pl.ds(0, lo + n - half), :]], axis=0))
        g = jnp.concatenate(pieces, axis=1)
        dw_ref[pl.ds(lo, n), :] = jnp.dot(
            g, x_mat[...], preferred_element_type=F32).astype(BF16)

    @pl.when(p < n_pp - 1)
    def _():
        for j in range(4):
            for xq in range(2):
                remote(
                    landed.at[j, xq], landed.at[j, xq], fs.at[0, 0], fr.at[j, xq],
                    partner).wait_recv()
            dx_ref[:, pl.ds(j * cols, cols)] = (
                landed[j, 0].astype(F32) + landed[j, 1].astype(F32)).astype(BF16)

    @pl.when(p == n_pp - 1)
    def _():
        dx_ref[...] = jnp.zeros_like(dx_ref)

    for k in (1, 2, 3):
        x_copy(k).wait_send()
    for k in range(nz):
        pair_copy(k).wait_send()
    for k in range(1, 5):
        for g in range(2):
            for c in ag_copies(g, k):
                c.wait_send()
        for plus in (True, False):
            for ri in range(4):
                rs_copy(plus, ri, k).wait_send()
    for plus in (True, False):
        g_copy(plus, 2).wait_send()

    g_sent(1)

    @pl.when(core == 1)
    def _():
        g_sent(0)


    @pl.when(p > 0)
    def _():
        for ri in range(4):
            for xq in range(2):
                fin_copy(ri, xq).wait_send()


def write_out(dx_v, dw_v, dx_hbm, dw_hbm, sem):
    copies = [
        pltpu.make_async_copy(dw_v, dw_hbm, sem.at[0]),
        pltpu.make_async_copy(dx_v, dx_hbm, sem.at[1]),
    ]
    for c in copies:
        c.start()
    for c in copies:
        c.wait()


def on_device(layer_input, gate_pre, up_pre, hidden_grad, gate_weight):
    x = layer_input[0, 0]
    gate, up, hid = (jnp.swapaxes(v[0, 0], 0, 1) for v in (gate_pre, up_pre, hidden_grad))
    w = jnp.swapaxes(gate_weight[0], 0, 1)
    hidden, toks = gate.shape
    cols = w.shape[1]
    half = (hidden // 2 + 15) // 16 * 16
    vm = pltpu.VMEM
    dma = pltpu.SemaphoreType.DMA
    dx, dw = pl.pallas_call(
        kernel,
        name="section",
        out_shape=(
            jax.ShapeDtypeStruct(x.shape, BF16),
            jax.ShapeDtypeStruct((hidden, cols), BF16),
        ),
        in_specs=[pl.BlockSpec(memory_space=pltpu.HBM)] * 5,
        out_specs=[pl.BlockSpec(memory_space=pltpu.VMEM)] * 2,
        scratch_shapes=[
            vm((hidden, toks), BF16), vm((hidden, toks), BF16), vm((hidden, toks), BF16),
            vm((hidden, cols), BF16),
            vm(x.shape, BF16),
            vm((4, 2, half, toks), BF16),
            vm((8, 2, 4, 8, cols), BF16),
            vm((512, cols), BF16),
            vm((4, 8, 16, cols), BF16),
            vm((2, 4, 4, 16, cols), BF16),
            vm((4, 2, 8, cols), BF16),
            vm((4, 2, 8, cols), BF16),
            dma((6,)), dma((3,)), dma((3,)), dma((8,)), dma((8,)),
            dma((2, 3)), dma((2, 3)),
            dma((2, 2, 4)), dma((2, 2, 4)),
            dma((2, 4, 4)), dma((2, 4, 4)),
            dma((4, 2)), dma((4, 2)), pltpu.SemaphoreType.REGULAR,
        ],
        compiler_params=pltpu.CompilerParams(
            collective_id=0, has_side_effects=True, vmem_limit_bytes=40 << 20),
    )(*(pltpu.with_memory_space_constraint(v, pltpu.HBM) for v in (x, gate, up, hid, w)))
    dx, dw = pl.pallas_call(
        write_out,
        name="write_out",
        out_shape=(
            jax.ShapeDtypeStruct(x.shape, BF16),
            jax.ShapeDtypeStruct((hidden, cols), BF16),
        ),
        in_specs=[pl.BlockSpec(memory_space=pltpu.VMEM)] * 2,
        out_specs=[pl.BlockSpec(memory_space=pltpu.HBM)] * 2,
        scratch_shapes=[dma((2,))],
        compiler_params=pltpu.CompilerParams(vmem_limit_bytes=8 << 20),
    )(dx, dw)
    return dx[None, None], jnp.swapaxes(dw, 0, 1)[None]


def solution(mesh):
    return jax.shard_map(
        on_device,
        mesh=mesh,
        in_specs=(
            P("pp", "dp", "tp", None),
            P("pp", "dp", None, "tp"),
            P("pp", "dp", None, "tp"),
            P("pp", "dp", None, "tp"),
            P("pp", "dp", "tp"),
        ),
        out_specs=(P("pp", "dp", "tp", None), P("pp", "dp", "tp")),
        check_vma=False,
    )
```
